128 devices in a mesh: row: 4 (over x_hi, core), col: 32 (over z, y, x_lo).
Axes of the slice: x: 4 (x_hi: 2, x_lo: 2; x = x_hi * 2 + x_lo), y: 4, z: 4, core: 2. Of those that a mesh axis runs over, the one named last changes fastest.
Arguments:
- rows: bfloat16 [4096, 4096], P(('row', 'col')), may hold values from -6 to 6
- task_ids: int32 [4096], P(('row', 'col')), may hold values from 0 to 8, as said below
- task_embed: bfloat16 [8, 4096], replicated, may hold values from -6 to 6
- norm_gain: float32 [4, 4096], replicated, may hold values from 0.1 to 1.9
- layer_weight: bfloat16 [4, 4096, 4096], P(None, None, 'col'), may hold values from -0.09375 to 0.09375
Outputs:
- packed_out: bfloat16 [4096, 4096], P('row', 'col')
The draws below stay inside these ranges and needn't reach their ends.
Inputs may be any that keep to these rules, and one draw needn't show every extreme that they name: `task_ids`: 8 marks an empty row, smaller values name a task.
All inputs are finite; a program needn't handle non-finite values.
Results may differ from the reference program's by a relative error of at most 0.008.
Values may be sent and summed in bfloat16 or wider, within the bound.
No kernel may reach another device: no remote copies, remote signals or barrier semaphores. Data moves between devices by JAX's collectives and lax.ppermute only.
A program may use at most 128 MiB of HBM per device.

```python
import jax
import jax.numpy as jnp
from jax import lax

D = 4096
N_TASK = 8
LAYERS = 4
ROWS_DEV = 32
ROWS_TOTAL = 4096
N_ROW = 4
N_COL = 32


def draw_task_ids(key, part):
    first_key, second_key = jax.random.split(jax.random.fold_in(key, 11))
    device_count = N_ROW * N_COL
    live_rows = jax.random.randint(first_key, (device_count, 1), 3 * ROWS_DEV // 4, ROWS_DEV + 1)
    picked = jax.random.randint(second_key, (device_count, ROWS_DEV), 0, N_TASK)
    positions = jnp.arange(ROWS_DEV, dtype=jnp.int32)[None, :]
    table = jnp.where(positions < live_rows, picked, N_TASK)
    return table.reshape(-1).astype(jnp.int32)


def block_levels(rng, extent, cuts, least, largest):
    loudness = 1.0
    for position, blocks in cuts:
        draws = jax.random.uniform(jax.random.fold_in(jax.random.fold_in(rng, 6), position), (blocks,), jnp.float32, least / len(cuts), largest / len(cuts))
        loudness = loudness * jnp.repeat(jnp.exp(draws), extent[position] // blocks).reshape((-1,) + (1,) * (len(extent) - 1 - position))
    return loudness


def gaussian(key, extent, width, limit, shards=(), kind=jnp.bfloat16):
    drawn = jax.random.normal(key, extent, jnp.float32) * width
    if len(shards) > 0:
        drawn = block_levels(key, extent, shards, -0.22, 0.18) * drawn
    return jnp.clip(drawn, min=-limit, max=limit).astype(kind)


def setup_inputs(seed: int = 0) -> dict:
    streams_of = jax.random.split(jax.random.key(seed), 6)
    rows = gaussian(streams_of[0], (ROWS_TOTAL, D), 1.0, 6.0, ((0, 128),))
    task_ids = draw_task_ids(jax.random.fold_in(streams_of[5], 71), 0)
    task_embed = gaussian(streams_of[2], (N_TASK, D), 1.0, 6.0)
    norm_gain = jnp.clip(1.0 + 0.18 * jax.random.normal(streams_of[3], (LAYERS, D), jnp.float32), 0.1, 1.9)
    layer_weight = gaussian(streams_of[4], (LAYERS, D, D), D ** -0.5, 0.09375, ((2, 32),))
    return {"rows": rows, "task_ids": task_ids, "task_embed": task_embed, "norm_gain": norm_gain, "layer_weight": layer_weight}


epsilon = 1e-06

def reference(rows, task_ids, task_embed, norm_gain, layer_weight):
    device_count = N_ROW * N_COL
    row_total = device_count * ROWS_DEV
    task_table = task_ids.reshape(device_count, ROWS_DEV)
    task_range = jnp.arange(N_TASK, dtype=jnp.int32)
    member = (task_table[:, :, None] == task_range[None, None, :]).astype(jnp.int32)
    counts = lax.optimization_barrier(jnp.sum(member, axis=1)).astype(jnp.int32)
    before = (jnp.cumsum(counts, axis=0) - counts).astype(jnp.int32)
    totals = lax.optimization_barrier(jnp.sum(counts, axis=0)).astype(jnp.int32)
    task_base = (jnp.cumsum(totals) - totals).astype(jnp.int32)
    task_rank = lax.optimization_barrier(jnp.sum(member * (jnp.cumsum(member, axis=1) - member), axis=2)).astype(jnp.int32)
    packed_pos = (lax.optimization_barrier(jnp.sum(member * (task_base[None, None, :] + before[:, None, :]), axis=2)) + task_rank).astype(jnp.int32)
    target = jnp.where(task_table < N_TASK, packed_pos, row_total).reshape(-1).astype(jnp.int32)
    packed = jnp.zeros((row_total, D), jnp.bfloat16).at[target].set(rows, mode='drop')
    slot_pos = jnp.arange(row_total, dtype=jnp.int32)
    in_task = (slot_pos[:, None] >= task_base[None, :]) & (slot_pos[:, None] < (task_base + totals)[None, :])
    task_term = jnp.dot(in_task.astype(jnp.bfloat16), task_embed, preferred_element_type=jnp.float32)
    hidden = (packed.astype(jnp.float32) + task_term).astype(jnp.bfloat16)
    hidden = hidden.reshape(ROWS_DEV * N_COL, N_ROW, D).transpose(1, 0, 2).reshape(row_total, D)
    for layer_index in range(LAYERS):
        values = hidden.astype(jnp.float32)
        inverse_rms = lax.rsqrt(lax.optimization_barrier(jnp.mean(values * values, axis=1, keepdims=True)) + epsilon)
        active = jax.nn.silu(values * inverse_rms * norm_gain[layer_index][None, :]).astype(jnp.bfloat16)
        update = jnp.dot(active, layer_weight[layer_index], preferred_element_type=jnp.float32)
        hidden = (values + update).astype(jnp.bfloat16)
    return hidden
```

```python
import jax
import jax.numpy as jnp
from jax import lax
from jax.experimental import pallas as pl
from jax.experimental.pallas import tpu as pltpu
from jax.sharding import Mesh
from jax.sharding import PartitionSpec as P

AXES = ("xh", "core", "z", "y", "xl")
COLS = ("z", "y", "xl")
PLANE = ("xh", "core", "y", "xl")
EPS = 1e-06
CAP = 56


def shift(x, axis, by):
    n = lax.axis_size(axis)
    return lax.ppermute(x, axis, [(i, (i + by) % n) for i in range(n)])


def near_x(x, which):
    pairs = [(0, 1), (1, 0), (2, 3), (3, 2)] if which == 0 else [(1, 2), (2, 1), (3, 0), (0, 3)]
    return lax.ppermute(x, ("xh", "xl"), pairs)


def swap_core(x):
    return lax.ppermute(x, "core", [(0, 1), (1, 0)])


def gather_weight(own):
    half = own.shape[0] // 2
    before = shift(own, "y", 1)
    after = shift(own, "y", -1)
    far_u = shift(before[:half], "y", 1)
    far_l = shift(after[half:], "y", -1)
    upper = jnp.stack([own[:half], before[:half], after[:half], far_u])
    lower = jnp.stack([own[half:], before[half:], after[half:], far_l])
    x_upper = near_x(upper, 0)
    x_lower = near_x(lower, 1)
    mine = (upper, x_upper, lower, x_lower)
    return mine + tuple(swap_core(a) for a in mine), far_l


def layer_kernel(first, *refs):
    where, own, before, after, far_u, far_l, gain = refs[:7]
    weights = refs[7:15]
    out = refs[15]
    raw, act, wbuf, sems = refs[16:]
    z, y, xl, core = where[0], where[1], where[2], where[3]
    copies = [
        pltpu.make_async_copy(w, wbuf.at[i], sems.at[i]) for i, w in enumerate(weights)
    ]
    for c in copies:
        c.start()
    zs = (z, lax.rem(z + 3, 4), lax.rem(z + 1, 4), lax.rem(z + 2, 4))
    if first:
        for ref, at in ((own, zs[0]), (before, zs[1]), (after, zs[2])):
            for k in range(4):
                raw[k, pl.ds(at * 32, 32), :] = ref[:, k * 1024 : (k + 1) * 1024]
        for ref, add in ((far_u, 0), (far_l, 16)):
            for k in range(4):
                raw[k, pl.ds(zs[3] * 32 + add, 16), :] = ref[:, k * 1024 : (k + 1) * 1024]
    else:
        raw[pl.ds(zs[0], 1)] = own[...][None]
        raw[pl.ds(zs[1], 1)] = before[...][None]
        raw[pl.ds(zs[2], 1)] = after[...][None]
        raw[pl.ds(zs[3], 1), :64, :] = far_u[...][None]
        raw[pl.ds(zs[3], 1), 64:, :] = far_l[...][None]
    total = jnp.zeros((128, 1), jnp.float32)
    for k in range(4):
        v = raw[k].astype(jnp.float32)
        total = total + jnp.sum(v * v, axis=1, keepdims=True)
    inv = lax.rsqrt(total * (1.0 / 4096.0) + EPS)
    for k in range(4):
        v = raw[k].astype(jnp.float32) * inv * gain[k]
        act[k] = (v / (1.0 + jnp.exp(-v))).astype(jnp.bfloat16)
    for c in copies:
        c.wait()
    parts = [act[pl.ds(q, 1)][0] for q in (2 * core, 2 * core + 1, 2 - 2 * core, 3 - 2 * core)]
    residual = raw.at[pl.ds(z, 1)]
    for d, by in enumerate((0, 3, 1, 2)):
        acc = jnp.zeros((128, 256), jnp.float32)
        for q in range(4):
            w = jnp.concatenate([wbuf[2 * q, d], wbuf[2 * q + 1, d]], axis=1)
            acc = acc + jnp.dot(parts[q], w, preferred_element_type=jnp.float32)
        base = lax.rem(y + by, 4) * 256
        for side, at in ((0, xl), (1, 1 - xl)):
            cols = pl.ds(pl.multiple_of(base + at * 128, 128), 128)
            h = residual[0, :, cols].astype(jnp.float32)
            out[:, cols] = (h + acc[:, side * 128 : (side + 1) * 128]).astype(jnp.bfloat16)


def layer(first, where, shards, gain, weights):
    vmem = pl.BlockSpec(memory_space=pltpu.VMEM)
    anywhere = pl.BlockSpec(memory_space=pl.ANY)
    return pl.pallas_call(
        lambda *refs: layer_kernel(first, *refs),
        out_shape=jax.ShapeDtypeStruct((128, 1024), jnp.bfloat16),
        in_specs=[pl.BlockSpec(memory_space=pltpu.SMEM)] + [vmem] * 6 + [anywhere] * 8,
        out_specs=vmem,
        scratch_shapes=[
            pltpu.VMEM((4, 128, 1024), jnp.bfloat16),
            pltpu.VMEM((4, 128, 1024), jnp.bfloat16),
            pltpu.VMEM((8, 4, 1024, 128), jnp.bfloat16),
            pltpu.SemaphoreType.DMA((8,)),
        ],
        compiler_params=pltpu.CompilerParams(vmem_limit_bytes=40 * 1024 * 1024),
        name="dense_layer",
    )(where, *shards, gain, *weights)


def ring(x):
    half = x.shape[0] // 2
    before = shift(x, "z", 1)
    after = shift(x, "z", -1)
    far_u = shift(before[:half], "z", 1)
    far_l = shift(after[half:], "z", -1)
    return x, before, after, far_u, far_l


def positions(ids, tasks):
    member = (ids.reshape(1, 32, 128) == jnp.arange(tasks, dtype=jnp.int32)[:, None, None])
    m = member.astype(jnp.bfloat16)
    lane = jnp.arange(128)
    tri = (lane[:, None] < lane[None, :]).astype(jnp.bfloat16)
    inside = jnp.dot(m.reshape(-1, 128), tri, preferred_element_type=jnp.float32)
    inside = inside.reshape(tasks, 32, 128)
    per_line = jnp.sum(m.astype(jnp.float32), axis=2)
    line = jnp.arange(32)
    lines = jnp.sum(
        jnp.where(line[None, None, :] < line[None, :, None], per_line[:, None, :], 0.0), axis=2
    )
    totals = jnp.sum(per_line, axis=1)
    task = jnp.arange(tasks)
    base = jnp.sum(jnp.where(task[None, :] < task[:, None], totals[None, :], 0.0), axis=1)
    pos = inside + (lines + base[:, None])[:, :, None]
    pos = jnp.sum(jnp.where(member, pos + 1.0, 0.0), axis=0) - 1.0
    return pos.astype(jnp.int32).reshape(-1)


def program(rows, task_ids, task_embed, norm_gain, layer_weight):
    tasks = task_embed.shape[0]
    layers = layer_weight.shape[0]
    xh, core, z, y, xl = (lax.axis_index(a) for a in AXES)
    where = jnp.stack([z, y, xl, core]).astype(jnp.int32)

    member = (task_ids[:, None] == jnp.arange(tasks, dtype=jnp.int32)[None, :])
    term = jnp.dot(member.astype(jnp.bfloat16), task_embed, preferred_element_type=jnp.float32)
    hidden = (rows.astype(jnp.float32) + term).astype(jnp.bfloat16)

    halves = lax.dynamic_slice_in_dim(layer_weight, core * 2048, 2048, 1)
    gains = norm_gain.reshape(layers, 4, 1, 1024)

    ids = lax.all_to_all(
        jnp.broadcast_to(task_ids[None], (128, 32)), AXES, 0, 0, tiled=True
    )
    pos = positions(ids.reshape(-1), tasks)
    live = pos >= 0
    by_group = pos.reshape(4, 4, 8, 32).transpose(0, 2, 1, 3).reshape(32, 128)
    target = jnp.where(by_group >= 0, by_group % 4, -1)
    j = jnp.arange(128)
    earlier = j[None, :, None] > j[None, None, :]
    order = jnp.sum(
        ((target[:, :, None] == target[:, None, :]) & earlier).astype(jnp.int32), axis=2
    )
    mine = (xh * 2 + core) * 8 + y * 2 + xl
    my_target = lax.dynamic_index_in_dim(target, mine, 0, keepdims=False)
    my_order = lax.dynamic_index_in_dim(order, mine, 0, keepdims=False)
    send_at = jnp.where(my_target >= 0, my_target * CAP + my_order, -1)
    select = (jnp.arange(4 * CAP)[:, None] == send_at[None, :]).astype(jnp.bfloat16)
    here = (target == xh * 2 + core)[:, None, :] & (
        order[:, None, :] == jnp.arange(CAP)[None, :, None]
    )
    slot = jnp.sum(jnp.where(here, by_group[:, None, :] // 4 + 1, 0), axis=2) - 1
    place = (jnp.arange(1024)[:, None] == slot.reshape(-1)[None, :]).astype(jnp.bfloat16)

    tied = halves[0]
    for l in range(layers):
        weights, last = gather_weight(tied)
        if l + 1 < layers:
            tied, _ = lax.optimization_barrier((halves[l + 1], last))
        hidden = layer(l == 0, where, ring(hidden), gains[l], weights)

    send = jnp.dot(select, hidden, preferred_element_type=jnp.float32).astype(jnp.bfloat16)
    send = send.reshape(4, CAP, 8, 128).transpose(0, 2, 1, 3).reshape(32, CAP, 128)
    got = lax.all_to_all(send, PLANE, 0, 0, tiled=True)
    return jnp.dot(
        place, got.reshape(32 * CAP, 128), preferred_element_type=jnp.float32
    ).astype(jnp.bfloat16)


def solution(mesh):
    finer = Mesh(mesh.devices.reshape(2, 2, 4, 4, 2), AXES)
    return jax.shard_map(
        program,
        mesh=finer,
        in_specs=(P(AXES, None), P(AXES), P(), P(), P(None, None, COLS)),
        out_specs=P(("xh", "core"), COLS),
        check_vma=False,
    )
```
